32 devices in a mesh: rows: 32 (over z, y, x, core).
Axes of the slice: x: 2, y: 2, z: 4, core: 2. Of those that a mesh axis runs over, the one named last changes fastest.
Arguments:
- a_mat: float32 [262144, 64], P('rows')
- b_mat: float32 [262144, 4], P('rows')
Outputs:
- output 1: float32 [262144, 64], P('rows')
- output 2: float32 [64, 64], replicated
- output 3: float32 [64, 4], replicated
All inputs are finite; a program needn't handle non-finite values.
Results may differ from the reference program's by a relative error of at most 0.001.
Values sent between devices are 32-bit elements.
A program may use at most 1 GiB of HBM per device.

```python
import jax
import jax.numpy as jnp

NUM_BLOCKS = 32
ROWS_DEV = 8192
COLS = 64
RHS = 4

TOTAL_ROWS = NUM_BLOCKS * ROWS_DEV


def setup_inputs(seed: int = 0) -> dict:
    key = jax.random.key(seed)
    key_gauss, key_weight, key_left, key_right, key_rhs = jax.random.split(key, 5)
    gauss = jax.random.normal(key_gauss, (NUM_BLOCKS, ROWS_DEV, COLS), jnp.float32)
    col_weight = jnp.exp(jax.random.normal(key_weight, (NUM_BLOCKS, 1, COLS), jnp.float32))
    col_weight = col_weight / jnp.sqrt(jnp.mean(col_weight * col_weight, axis=2, keepdims=True))
    left_rot = jnp.linalg.qr(jax.random.normal(key_left, (COLS, COLS), jnp.float32))[0]
    right_rot = jnp.linalg.qr(jax.random.normal(key_right, (COLS, COLS), jnp.float32))[0]
    spread = 10.0 ** jnp.linspace(0.0, -2.5, COLS, dtype=jnp.float32)
    spread = spread / jnp.sqrt(jnp.mean(spread * spread))
    mixing = jnp.dot(left_rot * spread[None, :], right_rot.T)
    weighted = (gauss * col_weight).reshape(TOTAL_ROWS, COLS)
    a_mat = jnp.dot(weighted, mixing) * (TOTAL_ROWS ** -0.5)
    b_mat = jax.random.normal(key_rhs, (TOTAL_ROWS, RHS), jnp.float32)
    return {'a_mat': a_mat, 'b_mat': b_mat}


def reference(a_mat, b_mat):
    q_raw, r_raw = jnp.linalg.qr(a_mat)
    diag_signs = jnp.sign(jnp.diagonal(r_raw))
    q_fac = q_raw * diag_signs[None, :]
    r_fac = r_raw * diag_signs[:, None]
    c_mat = jnp.dot(q_fac.T, b_mat, preferred_element_type=jnp.float32)
    return q_fac, r_fac, c_mat
```

```python
import functools

import jax
import jax.numpy as jnp
from jax import lax
from jax.experimental import pallas as pl
from jax.experimental.pallas import tpu as pltpu
from jax.sharding import PartitionSpec as P

FULL = lax.Precision.HIGHEST
MESH = pl.DeviceIdType.MESH
GROUP = 8
CHUNKS = 8
PIVOT_FLOOR = 1e-6


def dot_nt(a, b):
    return lax.dot_general(a, b, (((1,), (1,)), ((), ())), precision=FULL, preferred_element_type=jnp.float32)


def dot_nn(a, b):
    return lax.dot_general(a, b, (((1,), (0,)), ((), ())), precision=FULL, preferred_element_type=jnp.float32)


def fold(g):
    return jnp.concatenate([g[:32], g[32:]], axis=1)


def unfold_right(p):
    moved = pltpu.roll(p, 64, 1)
    both = jnp.concatenate([moved, p], axis=0)
    rows = lax.broadcasted_iota(jnp.int32, (64, 128), 0)
    cols = lax.broadcasted_iota(jnp.int32, (64, 128), 1)
    return jnp.where(cols < 64, jnp.where(rows == cols, 1.0, 0.0), both)


def factor(w):
    rows = lax.broadcasted_iota(jnp.int32, (64, 128), 0)
    cols = lax.broadcasted_iota(jnp.int32, (64, 128), 1)
    floor = jnp.sum(jnp.where(cols == rows + 64, w, 0.0), axis=1, keepdims=True) * PIVOT_FLOOR
    floor = jnp.broadcast_to(floor, (64, 128))
    row8 = lax.broadcasted_iota(jnp.int32, (8, 128), 0)
    col1 = lax.broadcasted_iota(jnp.int32, (1, 128), 1)
    done = []
    rest = w
    for blk in range(8):
        size = 64 - 8 * blk
        head, tail = rest[:8], (rest[8:] if size > 8 else None)
        lane = 64 + 8 * blk
        head_cols = [jnp.broadcast_to(head[:, lane + j:lane + j + 1], (8, 128)) for j in range(8)]
        tail_cols = None
        if tail is not None:
            tail_cols = [jnp.broadcast_to(tail[:, lane + j:lane + j + 1], (size - 8, 128)) for j in range(8)]
        for k in range(8):
            pivot = head_cols[k][k:k + 1]
            safe = jnp.maximum(pivot, floor[8 * blk + k:8 * blk + k + 1])
            scale = lax.rsqrt(safe)
            row = head[k:k + 1] + jnp.where(col1 == lane + k, safe - pivot, 0.0)
            row = row * scale
            below = jnp.where(row8 > k, head_cols[k] * scale, 0.0)
            head = jnp.where(row8 == k, row, head - below * row)
            if tail is not None:
                tail_k = tail_cols[k] * scale
                tail = tail - tail_k * row
            for j in range(k + 1, 8):
                entry = head_cols[j][k:k + 1] * scale
                head_cols[j] = head_cols[j] - below * entry
                if tail is not None:
                    tail_cols[j] = tail_cols[j] - tail_k * entry
        done.append(head)
        rest = tail
    return jnp.concatenate(done, axis=0)


def upper_of(y):
    moved = pltpu.roll(y, 64, 1)[:, :64]
    rows = lax.broadcasted_iota(jnp.int32, (64, 64), 0)
    cols = lax.broadcasted_iota(jnp.int32, (64, 64), 1)
    return jnp.where(rows <= cols, moved, 0.0)


def tree_sum(ref, count):
    terms = [ref[i] for i in range(count)]
    while len(terms) > 1:
        terms = [terms[i] + terms[i + 1] for i in range(0, len(terms), 2)]
    return terms[0]


def all_sum(part, near, far, near_send, near_recv, far_send, far_recv, devices):
    levels = devices // GROUP
    me = lax.axis_index('rows')
    slot, level = me % GROUP, me // GROUP
    near[slot] = part
    sends = []
    for step in range(GROUP - 1, 0, -1):
        peer = level * GROUP + (slot + step) % GROUP
        copy = pltpu.make_async_remote_copy(
            src_ref=near.at[slot], dst_ref=near.at[slot], send_sem=near_send.at[step], recv_sem=near_recv.at[slot],
            device_id=(peer,), device_id_type=MESH)
        copy.start()
        sends.append(copy)
    for step in range(1, GROUP):
        other = (slot + step) % GROUP
        pltpu.make_async_remote_copy(
            src_ref=near.at[other], dst_ref=near.at[other], send_sem=near_send.at[step], recv_sem=near_recv.at[other],
            device_id=(me,), device_id_type=MESH).wait_recv()
    far[level] = tree_sum(near, GROUP)
    for step in range(levels - 1, 0, -1):
        peer = ((level + step) % levels) * GROUP + slot
        copy = pltpu.make_async_remote_copy(
            src_ref=far.at[level], dst_ref=far.at[level], send_sem=far_send.at[step], recv_sem=far_recv.at[level],
            device_id=(peer,), device_id_type=MESH)
        copy.start()
        sends.append(copy)
    for step in range(1, levels):
        other = (level + step) % levels
        pltpu.make_async_remote_copy(
            src_ref=far.at[other], dst_ref=far.at[other], send_sem=far_send.at[step], recv_sem=far_recv.at[other],
            device_id=(me,), device_id_type=MESH).wait_recv()
    return tree_sum(far, levels), sends


def pass_kernel(devices, a_hbm, b_hbm, q_hbm, p_ref, r_ref, bad_ref, x_ref, b_ref, near1, far1, near2, far2,
                in_sem, b_sem, out_sem, *comm_sems):
    levels = devices // GROUP
    me = lax.axis_index('rows')
    slot, level = me % GROUP, me // GROUP
    rows = a_hbm.shape[1]
    size = rows // CHUNKS

    loads = []
    for i in range(CHUNKS):
        copy = pltpu.make_async_copy(
            a_hbm.at[:, pl.ds(i * size, size)], x_ref.at[pl.ds(0, 64), pl.ds(i * size, size)], in_sem.at[i])
        copy.start()
        loads.append(copy)
    load_b = pltpu.make_async_copy(b_hbm, b_ref, b_sem)
    load_b.start()

    barrier = pltpu.get_barrier_semaphore()
    for step in range(1, GROUP):
        pl.semaphore_signal(barrier, inc=1, device_id=(level * GROUP + (slot + step) % GROUP,), device_id_type=MESH)
    for step in range(1, levels):
        pl.semaphore_signal(barrier, inc=1, device_id=(((level + step) % levels) * GROUP + slot,), device_id_type=MESH)

    gram = jnp.zeros((64, 64), jnp.float32)
    for i in range(CHUNKS):
        loads[i].wait()
        x = x_ref[0:64, i * size:(i + 1) * size]
        gram = gram + dot_nt(x, x)

    pl.semaphore_wait(barrier, GROUP - 1 + levels - 1)
    total, sends = all_sum(fold(gram), near1, far1, *comm_sems[:4], devices)

    load_b.wait()
    y = factor(unfold_right(total))
    inv = y[:, :64]
    r_ref[...] = upper_of(y)

    acc = jnp.zeros((72, 64), jnp.float32)
    stores = []
    for i in range(CHUNKS):
        cols = slice(i * size, (i + 1) * size)
        q = dot_nn(inv, x_ref[0:64, cols])
        x_ref[0:64, cols] = q
        copy = pltpu.make_async_copy(
            x_ref.at[pl.ds(0, 64), pl.ds(i * size, size)], q_hbm.at[:, pl.ds(i * size, size)], out_sem.at[i])
        copy.start()
        stores.append(copy)
        both = jnp.concatenate([q, b_ref[:, cols], jnp.zeros((4, size), jnp.float32)], axis=0)
        acc = acc + dot_nt(both, q)

    part = jnp.concatenate([fold(acc[:64]), jnp.concatenate([acc[64:], jnp.zeros((8, 64), jnp.float32)], axis=1)], axis=0)
    total, more = all_sum(part, near2, far2, *comm_sems[4:], devices)
    p_ref[...] = total

    rows32 = lax.broadcasted_iota(jnp.int32, (32, 128), 0)
    cols32 = lax.broadcasted_iota(jnp.int32, (32, 128), 1)
    eye = jnp.where((cols32 == rows32) | (cols32 == rows32 + 96), 1.0, 0.0)
    off = total[:32] - eye
    bad_ref[...] = jnp.broadcast_to(jnp.sum(off * off), (1, 128))
    for copy in sends + more:
        copy.wait_send()
    for copy in stores:
        copy.wait()


def last_kernel(q1_hbm, p_ref, r1_ref, q_hbm, r_ref, c_ref, x_ref, in_sem, out_sem):
    rows = q1_hbm.shape[1]
    size = rows // CHUNKS
    loads = []
    for i in range(CHUNKS):
        copy = pltpu.make_async_copy(
            q1_hbm.at[:, pl.ds(i * size, size)], x_ref.at[:, pl.ds(i * size, size)], in_sem.at[i])
        copy.start()
        loads.append(copy)
    y = factor(unfold_right(p_ref[0:32, :]))
    inv = y[:, :64]
    stores = []
    for i in range(CHUNKS):
        loads[i].wait()
        cols = slice(i * size, (i + 1) * size)
        x_ref[:, cols] = dot_nn(inv, x_ref[:, cols])
        copy = pltpu.make_async_copy(
            x_ref.at[:, pl.ds(i * size, size)], q_hbm.at[:, pl.ds(i * size, size)], out_sem.at[i])
        copy.start()
        stores.append(copy)
    r_ref[...] = dot_nn(upper_of(y), r1_ref[...])
    c_ref[...] = dot_nt(p_ref[32:40, 0:64], inv)[:4]
    for copy in stores:
        copy.wait()


def solution(mesh):
    devices = mesh.shape['rows']
    levels = devices // GROUP
    any_spec = pl.BlockSpec(memory_space=pl.ANY)
    vmem_spec = pl.BlockSpec(memory_space=pltpu.VMEM)
    f32 = jnp.float32
    dma = pltpu.SemaphoreType.DMA

    def one_pass(x, b):
        rows = x.shape[1]
        return pl.pallas_call(
            functools.partial(pass_kernel, devices),
            out_shape=[
                jax.ShapeDtypeStruct((64, rows), f32), jax.ShapeDtypeStruct((40, 128), f32),
                jax.ShapeDtypeStruct((64, 64), f32), jax.ShapeDtypeStruct((1, 128), f32)],
            in_specs=[any_spec, any_spec],
            out_specs=[any_spec, vmem_spec, vmem_spec, vmem_spec],
            scratch_shapes=[
                pltpu.VMEM((64, rows), f32), pltpu.VMEM((4, rows), f32),
                pltpu.VMEM((GROUP, 32, 128), f32), pltpu.VMEM((levels, 32, 128), f32),
                pltpu.VMEM((GROUP, 40, 128), f32), pltpu.VMEM((levels, 40, 128), f32),
                dma((CHUNKS,)), dma, dma((CHUNKS,)),
                dma((GROUP,)), dma((GROUP,)), dma((levels,)), dma((levels,)),
                dma((GROUP,)), dma((GROUP,)), dma((levels,)), dma((levels,))],
            compiler_params=pltpu.CompilerParams(collective_id=0, has_side_effects=True),
            name='gram_pass',
        )(x, b)

    def last(q1, p, r1):
        rows = q1.shape[1]
        return pl.pallas_call(
            last_kernel,
            out_shape=[
                jax.ShapeDtypeStruct((64, rows), f32), jax.ShapeDtypeStruct((64, 64), f32),
                jax.ShapeDtypeStruct((4, 64), f32)],
            in_specs=[any_spec, vmem_spec, vmem_spec],
            out_specs=[any_spec, vmem_spec, vmem_spec],
            scratch_shapes=[pltpu.VMEM((64, rows), f32), dma((CHUNKS,)), dma((CHUNKS,))],
            name='last_pass',
        )(q1, p, r1)

    def local_fn(a_blk, b_blk):
        b_t = b_blk.T
        q1, p, r1, bad = one_pass(a_blk.T, b_t)

        def again(state):
            q1, p, r1, bad = state
            q2, p, r2, bad = one_pass(q1, b_t)
            return q2, p, jnp.dot(r2, r1, precision=FULL), bad

        q1, p, r1, bad = lax.while_loop(lambda state: state[3][0, 0] > 0.25, again, (q1, p, r1, bad))
        q, r_fac, c = last(q1, p, r1)
        return q.T, r_fac, c.T

    return jax.shard_map(local_fn, mesh=mesh, in_specs=(P('rows', None), P('rows', None)),
                         out_specs=(P('rows', None), P(), P()), check_vma=False)
```
